128 devices in a mesh: pair: 32 (over x, y, z_lo), idx: 4 (over z_hi, core).
Axes of the slice: x: 4, y: 4, z: 4 (z_hi: 2, z_lo: 2; z = z_hi * 2 + z_lo), core: 2. Of those that a mesh axis runs over, the one named last changes fastest.
Arguments:
- g2: bfloat16 [512, 512, 2, 1, 512], P('pair', None, None, None, 'idx'), may hold values from -6 to 6
- core_ham: float32 [512, 512], replicated, may hold values from -0.25 to 0.25
- dipole: float32 [512, 512], replicated, may hold values from -0.125 to 0.125
- field: float32 [1], replicated, may hold values from 0.5 to 1.5
- rho: bfloat16 [2, 512, 512], replicated, may hold values from -6 to 6
- factors: bfloat16 [2048, 512, 512], P(None, 'pair', 'idx'), may hold values from -0.046875 to 0.046875
- damping: float32 [512], replicated, may hold values from 0.02 to 0.2
Outputs:
- g2_next: bfloat16 [512, 512, 2, 1, 512], P('pair', None, None, None, 'idx')
The draws below stay inside these ranges and needn't reach their ends.
All inputs are finite; a program needn't handle non-finite values.
Results may differ from the reference program's by a relative error of at most 0.0056.
Values may be sent and summed in bfloat16 or wider, within the bound.
No kernel may reach another device: no remote copies, remote signals or barrier semaphores. Data moves between devices by JAX's collectives and lax.ppermute only.
A program may use at most 192 MiB of HBM per device.

```python
import math
import jax
import jax.numpy as jnp
from jax import lax

N = 512
Q = 2048
JS = 1


def block_scale(key, dims, shards, low, largest):
    gain = 1.0
    for axis_at, parts in shards:
        heights = jax.random.uniform(jax.random.fold_in(jax.random.fold_in(key, 6), axis_at), (parts,), jnp.float32, low / len(shards), largest / len(shards))
        gain = gain * jnp.repeat(jnp.exp(heights), dims[axis_at] // parts).reshape((-1,) + (1,) * (len(dims) - 1 - axis_at))
    return gain


def normal_values(rng, extent, deviation, most, split=(), kind=jnp.bfloat16):
    gain = block_scale(rng, extent, split, -0.22, 0.18) if split else 1.0
    drawn = jax.random.normal(rng, extent, jnp.float32) * deviation * gain
    return jnp.minimum(jnp.maximum(drawn, -most), most).astype(kind)


def setup_inputs(seed: int = 0) -> dict:
    key_list = jax.random.split(jax.random.key(seed), 8)
    g2 = normal_values(key_list[0], (N, N, 2, JS, N), 1.0, 6.0, ((0, 32), (4, 4)))
    core_ham = normal_values(key_list[1], (N, N), N ** -0.5, 0.25, (), jnp.float32)
    dipole = normal_values(key_list[2], (N, N), (4 * N) ** -0.5, 0.125, (), jnp.float32)
    field = jnp.clip(jax.random.uniform(key_list[3], (1,), jnp.float32, 0.5, 1.5), 0.5, 1.5)
    rho = normal_values(key_list[4], (2, N, N), 1.0, 6.0)
    factors = normal_values(key_list[5], (Q, N, N), (32 * N) ** -0.5, 0.046875, ((1, 32), (2, 4)))
    damping = jnp.clip(jnp.exp(jax.random.uniform(key_list[6], (N,), jnp.float32, math.log(0.02), math.log(0.2))), 0.02, 0.2)
    return {"g2": g2, "core_ham": core_ham, "dipole": dipole, "field": field, "rho": rho, "factors": factors, "damping": damping}


def combine(total_x, total_z, rho_part):
    real = total_z[:, 0, None, None] * rho_part[0][None] - total_z[:, 1, None, None] * rho_part[1][None]
    imag = total_z[:, 0, None, None] * rho_part[1][None] + total_z[:, 1, None, None] * rho_part[0][None]
    return total_x + jnp.stack([real, imag], axis=1)


def reference(g2, core_ham, dipole, field, rho, factors, damping):
    step_size = 1.0
    hamil = 0.5 * (core_ham + core_ham.T) + field[0] * (0.5 * (dipole + dipole.T))
    ham_b = hamil.astype(jnp.bfloat16)
    ham_f = ham_b.astype(jnp.float32)
    slab_ham = ham_f[:JS, :JS]
    term_i = jnp.dot(ham_b, g2.reshape(N, -1), preferred_element_type=jnp.float32).astype(jnp.bfloat16).reshape(g2.shape)
    lflat = factors.reshape(Q, N * N)
    xsum = jnp.dot(lflat, g2.reshape(N * N, -1), preferred_element_type=jnp.float32)
    zsum = lax.dot_general(lflat, rho.reshape(2, N * N), (((1,), (1,)), ((), ())), preferred_element_type=jnp.float32)
    slab_rho = rho[:, :JS, :].astype(jnp.float32)
    aux = combine(xsum.reshape(Q, 2, JS, N), zsum, slab_rho).astype(jnp.bfloat16)
    aux_flat = aux.reshape(Q, -1)
    blocks = 8
    size_b = N // blocks

    def one_block(start):
        start = start.astype(jnp.int32)
        group_g = lax.dynamic_slice_in_dim(g2, start, size_b, 0)
        group_i = lax.dynamic_slice_in_dim(term_i, start, size_b, 0)
        lmat = lax.dynamic_slice_in_dim(factors, start, size_b, 1).reshape(Q, -1)
        gam_rows = lax.dynamic_slice_in_dim(damping, start, size_b, 0)
        ham_cols = jnp.dot(group_g.reshape(-1, N), ham_b, preferred_element_type=jnp.float32).reshape(group_g.shape)
        factor_term = lax.dot_general(lmat, aux_flat, (((0,), (0,)), ((), ())), preferred_element_type=jnp.float32).reshape(group_g.shape)
        part_two = (factor_term - ham_cols).astype(jnp.bfloat16)
        values = group_g.astype(jnp.float32)
        term_k = jnp.einsum("km,imr->ikr", ham_f, values.reshape(size_b, N, -1)).reshape(group_g.shape)
        term_j = jnp.einsum("jm,ikcml->ikcjl", slab_ham, values)
        rate = group_i.astype(jnp.float32) + part_two.astype(jnp.float32) + term_j - term_k
        decay = gam_rows[:, None, None, None] + damping[None, :, None, None] + damping[:JS][None, None, :, None] + damping[None, None, None, :]
        real_next = values[:, :, 0] + step_size * rate[:, :, 1] - step_size * decay * values[:, :, 0]
        imag_next = values[:, :, 1] - step_size * rate[:, :, 0] - step_size * decay * values[:, :, 1]
        return jnp.stack([real_next, imag_next], axis=2).astype(jnp.bfloat16)

    starts = jnp.arange(blocks, dtype=jnp.int32) * size_b
    result = lax.map(one_block, starts)
    return result.reshape(g2.shape)
```

```python
import functools

import jax
import jax.numpy as jnp
from jax import lax
from jax.experimental import pallas as pl
from jax.experimental.pallas import tpu as pltpu
from jax.sharding import Mesh, PartitionSpec as P

F32 = jnp.float32
BF16 = jnp.bfloat16
CHIP = ("x", "y", "zl", "zh")


def shape(dims, dtype=BF16):
    return jax.ShapeDtypeStruct(dims, dtype)


def call(body, out, grid, ins, outs, scratch, flops, moved, prefetch=1, **kw):
    return pl.pallas_call(
        body,
        out_shape=out,
        grid_spec=pltpu.PrefetchScalarGridSpec(
            num_scalar_prefetch=prefetch,
            grid=grid,
            in_specs=ins,
            out_specs=outs,
            scratch_shapes=scratch,
        ),
        compiler_params=pltpu.CompilerParams(
            dimension_semantics=("arbitrary",) * len(grid), vmem_limit_bytes=56 << 20
        ),
        cost_estimate=pl.CostEstimate(flops=flops, bytes_accessed=moved, transcendentals=0),
        **kw,
    )


def hold(step, first, count):
    return jnp.clip(step - first, 0, count - 1)


def split_body(me, g, t_out, e0, e1, e2, e3, scr):
    step = pl.program_id(0)
    for sub in range(4):
        for i in range(16):
            scr[pl.ds(i * 40, 32), :] = g[i, sub * 32 : sub * 32 + 32, :].astype(F32)
        for kc in range(32):
            t_out[sub, kc] = scr[pl.ds(kc, 16, stride=40), :].astype(BF16)
        for s, e in enumerate((e0, e1, e2, e3)):

            @pl.when(step // 2 == s)
            def _(e=e, sub=sub):
                for c in range(2):
                    for i in range(16):
                        rows = scr[pl.ds(i * 40 + c, 16, stride=2), :]
                        e[c, i, sub * 16 : sub * 16 + 16, :] = rows.astype(BF16)


def split(me, g):
    def where(t, me):
        return jnp.bitwise_xor(me[0], t // 2) * 2 + t % 2

    piece = lambda s: pl.BlockSpec((2, 16, 64, 128), lambda t, me: (0, 0, hold(t, 2 * s, 2), 0))
    return call(
        split_body,
        (shape((32, 32, 16, 128)),) + (shape((2, 16, 128, 128)),) * 4,
        (8,),
        [pl.BlockSpec((16, 128, 128), lambda t, me: (0, where(t, me), 0))],
        (pl.BlockSpec((4, 32, 16, 128), lambda t, me: (where(t, me), 0, 0, 0)),)
        + tuple(piece(s) for s in range(4)),
        [pltpu.VMEM((640, 128), F32)],
        1 << 24,
        12 << 20,
    )(me, g)


def turn_body(me, l, la, lt, scr):
    @pl.loop(0, 128)
    def _(q):
        scr[pl.ds(pl.multiple_of(q * 24, 8), 16), :] = l[q].astype(F32)

    for m in range(16):
        rows = scr[pl.ds(m, 128, stride=24), :]
        la[:, m * 128 : m * 128 + 128] = rows.astype(BF16)
        lt[m * 128 : m * 128 + 128, :] = rows.T.astype(BF16)


def turn(me, factors):
    return call(
        turn_body,
        (shape((2048, 2048)), shape((2048, 2048))),
        (16,),
        [pl.BlockSpec((128, 16, 128), lambda t, me: (t, 0, 0))],
        (
            pl.BlockSpec((128, 2048), lambda t, me: (t, 0)),
            pl.BlockSpec((2048, 128), lambda t, me: (0, t)),
        ),
        [pltpu.VMEM((3072, 128), F32)],
        1 << 26,
        24 << 20,
    )(me, factors)


def base_body(me, e0, e1, e2, e3, ham, dk, dl, di, out, scr):
    for s, e in enumerate((e0, e1, e2, e3)):
        at = pl.multiple_of(jnp.bitwise_xor(me[0], s) * 128, 128)
        for c in range(2):
            scr[pl.ds(at, 128), c * 128 : c * 128 + 128] = e[c, 0]
    term_k = jnp.dot(ham[...], scr[...], preferred_element_type=F32)
    real = scr[:, :128].astype(F32)
    imag = scr[:, 128:].astype(F32)
    h00 = ham[0:1, 0:1].astype(F32)
    decay = di[0] + dk[...] + dl[...]
    out[0, 0] = real + (h00 * imag - term_k[:, 128:]) - decay * real
    out[1, 0] = imag - (h00 * real - term_k[:, :128]) - decay * imag


def base(me, pieces, ham, dk, dl, di):
    return call(
        base_body,
        shape((2, 16, 512, 128), F32),
        (16,),
        [pl.BlockSpec((2, 1, 128, 128), lambda t, me: (0, t, 0, 0))] * 4
        + [
            pl.BlockSpec((512, 512), lambda t, me: (0, 0)),
            pl.BlockSpec((512, 1), lambda t, me: (0, 0)),
            pl.BlockSpec((1, 128), lambda t, me: (0, 0)),
            pl.BlockSpec((1, 1, 1), lambda t, me: (t, 0, 0)),
        ],
        pl.BlockSpec((2, 1, 512, 128), lambda t, me: (0, t, 0, 0)),
        [pltpu.VMEM((512, 256), BF16)],
        1 << 31,
        12 << 20,
    )(me, *pieces, ham, dk, dl, di)


def project_body(me, la, w0, w1, w2, w3, z, rho, out, scr):
    @pl.when(pl.program_id(0) == 0)
    def _():
        for s, w in enumerate((w0, w1, w2, w3)):
            at = jnp.bitwise_xor(me[0], s) * 128
            for c in range(2):
                scr[:, pl.ds(pl.multiple_of(at + c * 512, 128), 128)] = w[c]

    zr, zi = z[:, 0:1], z[:, 1:2]
    for n in range(4):
        cols = slice((n % 2) * 256, (n % 2) * 256 + 256)
        x = jnp.dot(la[...], scr[:, n * 256 : n * 256 + 256], preferred_element_type=F32)
        rr, ri = rho[0:1, cols], rho[1:2, cols]
        x += zr * rr - zi * ri if n < 2 else zr * ri + zi * rr
        out[:, n * 256 : n * 256 + 256] = x.astype(out.dtype)


def project(me, la, pieces, z, rho, other, dtype):
    def at(t, me):
        half = me[0] % 2
        return ((1 - half if other else half) * 4 + t, 0)

    return call(
        project_body,
        shape((1024, 1024), dtype),
        (4,),
        [pl.BlockSpec((256, 2048), at)]
        + [pl.BlockSpec((2, 2048, 128), lambda t, me: (0, 0, 0))] * 4
        + [pl.BlockSpec((256, 2), at), pl.BlockSpec((2, 512), lambda t, me: (0, 0))],
        pl.BlockSpec((256, 1024), lambda t, me: (t, 0)),
        [pltpu.VMEM((2048, 1024), BF16)],
        1 << 32,
        10 << 20,
    )(me, la, *pieces, z, rho)


def second_body(me, lt, own, oth, w0, w1, w2, w3, ham, o0, o1, o2, o3, wcat, res):
    half = me[0] % 2
    lt_own = lt[:, pl.ds(pl.multiple_of(half * 1024, 128), 1024)]
    lt_oth = lt[:, pl.ds(pl.multiple_of((1 - half) * 1024, 128), 1024)]
    for c in range(2):
        for s, w in enumerate((w0, w1, w2, w3)):
            at = jnp.bitwise_xor(me[0], s) * 128
            wcat[:, pl.ds(pl.multiple_of(at, 128), 128)] = w[c]
        for n in range(2):
            cols = slice(c * 512 + n * 256, c * 512 + n * 256 + 256)
            y = jnp.dot(lt_own, own[:, cols], preferred_element_type=F32)
            y += jnp.dot(lt_oth, oth[:, cols], preferred_element_type=F32)
            y -= jnp.dot(wcat[...], ham[:, n * 256 : n * 256 + 256], preferred_element_type=F32)
            res[:, cols] = y.astype(BF16)
        for s, o in enumerate((o0, o1, o2, o3)):
            at = jnp.bitwise_xor(me[0], s) * 128 + c * 512
            o[c] = res[:, pl.ds(pl.multiple_of(at, 128), 128)]


def second(me, lt, own, oth, pieces, ham, first, steps):
    return call(
        second_body,
        (shape((2, steps * 256, 128)),) * 4,
        (steps,),
        [
            pl.BlockSpec((256, 2048), lambda t, me: (t + first, 0)),
            pl.BlockSpec((1024, 1024), lambda t, me: (0, 0)),
            pl.BlockSpec((1024, 1024), lambda t, me: (0, 0)),
        ]
        + [pl.BlockSpec((2, 256, 128), lambda t, me: (0, t + first, 0))] * 4
        + [pl.BlockSpec((512, 512), lambda t, me: (0, 0))],
        (pl.BlockSpec((2, 256, 128), lambda t, me: (0, t, 0)),) * 4,
        [pltpu.VMEM((256, 512), BF16), pltpu.VMEM((256, 1024), BF16)],
        1 << 32,
        14 << 20,
    )(me, lt, own, oth, *pieces, ham)


def mix_body(me, part, ham, out):
    for j in range(4):
        left = part[:, 2 * j].reshape(512, 128)
        right = part[:, 2 * j + 1].reshape(512, 128)
        both = jnp.concatenate([left, right], axis=1)
        y = jnp.dot(ham[...], both, preferred_element_type=F32).astype(BF16)
        out[:, 2 * j] = y[:, :128].reshape(32, 16, 128)
        out[:, 2 * j + 1] = y[:, 128:].reshape(32, 16, 128)


def mix(me, part, ham):
    return call(
        mix_body,
        shape((32, 32, 16, 128)),
        (4,),
        [
            pl.BlockSpec((32, 8, 16, 128), lambda t, me: (0, t, 0, 0)),
            pl.BlockSpec((512, 512), lambda t, me: (0, 0)),
        ],
        pl.BlockSpec((32, 8, 16, 128), lambda t, me: (0, t, 0, 0)),
        [],
        1 << 31,
        8 << 20,
    )(me, part, ham)


def add_body(me, t, b, out, scr):
    for sub in range(4):
        for c in range(2):
            for k in range(16):
                scr[pl.ds((c * 16 + k) * 24, 16), :] = t[sub, 2 * k + c].astype(F32)
        rows = slice(sub * 16, sub * 16 + 16)
        for i in range(16):
            real = scr[pl.ds(i, 16, stride=24), :]
            imag = scr[pl.ds(384 + i, 16, stride=24), :]
            out[0, i, rows, :] = b[0, i, rows, :] + imag
            out[1, i, rows, :] = b[1, i, rows, :] - real


def add(me, t, b):
    spec = pl.BlockSpec((2, 16, 64, 128), lambda t, me: (0, 0, t, 0))
    return call(
        add_body,
        shape((2, 16, 512, 128), F32),
        (8,),
        [pl.BlockSpec((4, 32, 16, 128), lambda t, me: (t, 0, 0, 0)), spec],
        spec,
        [pltpu.VMEM((768, 128), F32)],
        1 << 24,
        20 << 20,
    )(me, t, b)


def finish_body(me, b, *refs):
    pieces, out, scr = refs[:8], refs[8], refs[9]
    step = pl.program_id(0)
    for s in range(4):

        @pl.when(step // 2 == s)
        def _(s=s):
            for sub in range(4):
                rows = slice(sub * 16, sub * 16 + 16)
                for i in range(16):
                    v = pieces[2 * s + i // 8]
                    real = b[0, i, rows, :] + v[1, i % 8, rows, :].astype(F32)
                    imag = b[1, i, rows, :] - v[0, i % 8, rows, :].astype(F32)
                    scr[pl.ds(i * 40, 16, stride=2), :] = real
                    scr[pl.ds(i * 40 + 1, 16, stride=2), :] = imag
                for i in range(16):
                    block = scr[pl.ds(i * 40, 32), :].astype(BF16)
                    out[i, sub * 32 : sub * 32 + 32, :] = block


def finish(me, b, pieces):
    def where(t, me):
        return jnp.bitwise_xor(me[0], t // 2) * 2 + t % 2

    piece = lambda s: pl.BlockSpec((2, 8, 64, 128), lambda t, me: (0, 0, hold(t, 2 * s, 2), 0))
    return call(
        finish_body,
        shape((16, 1024, 128)),
        (8,),
        [pl.BlockSpec((2, 16, 64, 128), lambda t, me: (0, 0, where(t, me), 0))]
        + [piece(s) for s in range(4) for _ in range(2)],
        pl.BlockSpec((16, 128, 128), lambda t, me: (0, where(t, me), 0)),
        [pltpu.VMEM((640, 128), F32)],
        1 << 24,
        16 << 20,
    )(me, b, *pieces)


def swap(v, s):
    return lax.ppermute(v, ("zh", "c"), [(d, d ^ s) for d in range(4)])


def to_owner(v, axes):
    return lax.all_to_all(v, axes, split_axis=0, concat_axis=0, tiled=True)


def per_device(g2, core_ham, dipole, field, rho, factors, damping):
    rows, width, _, _, cols = g2.shape
    pair = ("x", "y", "zl")
    pair_at = lax.axis_index(pair)
    idx_at = lax.axis_index(("zh", "c"))
    me = idx_at.astype(jnp.int32).reshape(1)

    t, *e = split(me, g2.reshape(rows, width * 2, cols))
    w = [e[0]] + [swap(e[s], s) for s in (1, 2, 3)]
    w = [v.reshape(2, rows * 128, cols) for v in w]

    hamil = 0.5 * (core_ham + core_ham.T) + field[0] * (0.5 * (dipole + dipole.T))
    ham = hamil.astype(BF16)
    part = to_owner(t, pair)

    rho_rows = lax.dynamic_slice_in_dim(rho, pair_at * rows, rows, 1)
    rho_local = lax.dynamic_slice_in_dim(rho_rows, idx_at * cols, cols, 2)
    z = lax.dot_general(
        factors, rho_local, (((1, 2), (1, 2)), ((), ())), preferred_element_type=F32
    )
    slab = rho[:, 0, :].astype(F32)
    la, lt = turn(me, factors)
    di = lax.dynamic_slice_in_dim(damping, pair_at * rows, rows, 0) + damping[0]
    dl = lax.dynamic_slice_in_dim(damping, idx_at * cols, cols, 0).reshape(1, cols)
    b = base(me, e, ham, damping.reshape(width, 1), dl, di.reshape(rows, 1, 1))

    theirs = project(me, la, w, z, slab, True, BF16)
    theirs = swap(theirs, 1)
    mine = project(me, la, w, z, slab, False, F32)
    share = (mine + theirs.astype(F32)).astype(BF16).reshape(64, 16, 1024)
    share = to_owner(share, CHIP)
    aux = jnp.sum(share.astype(F32), axis=0).astype(BF16)
    own = to_owner(jnp.broadcast_to(aux[None], share.shape), CHIP).reshape(1024, 1024)
    oth = swap(own, 1)

    mixed = mix(me, part, ham)
    b = add(me, to_owner(mixed, pair), b)

    halves = []
    for h in range(2):
        r = second(me, lt, own, oth, w, ham, 4 * h, 4)
        halves.append([r[0]] + [swap(r[s], s) for s in (1, 2, 3)])
    pieces = [halves[h][s].reshape(2, 8, 128, cols) for s in range(4) for h in range(2)]
    out = finish(me, b, pieces)
    return out.reshape(rows, width, 2, 1, cols)


def solution(mesh):
    fine = Mesh(mesh.devices.reshape(4, 4, 2, 2, 2), ("x", "y", "zl", "zh", "c"))
    pair, idx = ("x", "y", "zl"), ("zh", "c")
    placed = (P(pair, None, None, None, idx), P(), P(), P(), P(), P(None, pair, idx), P())
    return jax.shard_map(
        per_device,
        mesh=fine,
        in_specs=placed,
        out_specs=P(pair, None, None, None, idx),
        check_vma=False,
    )
```

```python
import functools

import jax
import jax.numpy as jnp
from jax import lax
from jax.experimental import pallas as pl
from jax.experimental.pallas import tpu as pltpu
from jax.sharding import Mesh, PartitionSpec as P

F32 = jnp.float32
BF16 = jnp.bfloat16


def shape(dims, dtype=BF16):
    return jax.ShapeDtypeStruct(dims, dtype)


def call(body, out, grid, ins, outs, scratch, flops, moved, prefetch=1, **kw):
    return pl.pallas_call(
        body,
        out_shape=out,
        grid_spec=pltpu.PrefetchScalarGridSpec(
            num_scalar_prefetch=prefetch,
            grid=grid,
            in_specs=ins,
            out_specs=outs,
            scratch_shapes=scratch,
        ),
        compiler_params=pltpu.CompilerParams(
            dimension_semantics=("arbitrary",) * len(grid), vmem_limit_bytes=56 << 20
        ),
        cost_estimate=pl.CostEstimate(flops=flops, bytes_accessed=moved, transcendentals=0),
        **kw,
    )


def hold(step, first, count):
    return jnp.clip(step - first, 0, count - 1)


def pick_body(me, g, e0, e1, scr):
    step = pl.program_id(0)
    for sub in range(4):
        for i in range(16):
            scr[pl.ds(i * 40, 32), :] = g[i, sub * 32 : sub * 32 + 32, :].astype(F32)
        for s, e in enumerate((e0, e1)):

            @pl.when(step // 2 == s)
            def _(e=e, sub=sub):
                for c in range(2):
                    for i in range(16):
                        rows = scr[pl.ds(i * 40 + c, 16, stride=2), :]
                        e[c, i, sub * 16 : sub * 16 + 16, :] = rows.astype(BF16)


def pick(me, g, first):
    def where(t, me):
        return jnp.bitwise_xor(me[0], first + t // 2) * 2 + t % 2

    piece = lambda s: pl.BlockSpec((2, 16, 64, 128), lambda t, me: (0, 0, hold(t, 2 * s, 2), 0))
    return call(
        pick_body,
        (shape((2, 16, 128, 128)),) * 2,
        (4,),
        [pl.BlockSpec((16, 128, 128), lambda t, me: (0, where(t, me), 0))],
        (piece(0), piece(1)),
        [pltpu.VMEM((640, 128), F32)],
        1 << 24,
        4 << 20,
    )(me, g)


def deal_body(me, *refs):
    gs, t_out, scr = refs[:4], refs[4], refs[5]
    for sub, g in enumerate(gs):
        for i in range(16):
            scr[pl.ds(i * 40, 32), :] = g[i].astype(F32)
        for kc in range(32):
            t_out[sub, kc] = scr[pl.ds(kc, 16, stride=40), :].astype(BF16)


def side_of(me, other):
    return 1 - me[1] if other else me[1]


def deal(me, g, other):
    def piece(sub):
        at = lambda t, me: (0, (t * 4 + sub) * 2 + side_of(me, other), 0)
        return pl.BlockSpec((16, 32, 128), at)

    return call(
        deal_body,
        shape((16, 32, 16, 128)),
        (4,),
        [piece(sub) for sub in range(4)],
        pl.BlockSpec((4, 32, 16, 128), lambda t, me: (t, 0, 0, 0)),
        [pltpu.VMEM((640, 128), F32)],
        1 << 24,
        4 << 20,
    )(me, g, g, g, g)


def flat_body(me, l, la, scr):
    for q in range(128):
        scr[pl.ds(q * 24, 16), :] = l[q].astype(F32)
    for m in range(16):
        rows = scr[pl.ds(m, 128, stride=24), :]
        la[:, m * 128 : m * 128 + 128] = rows.astype(BF16)


def flat(me, factors):
    return call(
        flat_body,
        shape((2048, 2048)),
        (16,),
        [pl.BlockSpec((128, 16, 128), lambda t, me: (t, 0, 0))],
        pl.BlockSpec((128, 2048), lambda t, me: (t, 0)),
        [pltpu.VMEM((3072, 128), F32)],
        1 << 24,
        16 << 20,
    )(me, factors)


def turn_body(me, la, lt):
    for m in range(8):
        lt[m * 128 : m * 128 + 128, :] = la[:, m * 128 : m * 128 + 128].T


def turn(me, la):
    return call(
        turn_body,
        shape((2048, 2048)),
        (2, 8),
        [pl.BlockSpec((256, 1024), lambda r, t, me: (t, r))],
        pl.BlockSpec((1024, 256), lambda r, t, me: (r, t)),
        [],
        1 << 26,
        16 << 20,
    )(me, la)


def base_body(me, e0, e1, e2, e3, ham, dk, dl, di, out, scr):
    for s, e in enumerate((e0, e1, e2, e3)):
        at = pl.multiple_of(jnp.bitwise_xor(me[0], s) * 128, 128)
        for c in range(2):
            scr[pl.ds(at, 128), c * 128 : c * 128 + 128] = e[c, 0]
    term_k = jnp.dot(ham[...], scr[...], preferred_element_type=F32)
    real = scr[:, :128].astype(F32)
    imag = scr[:, 128:].astype(F32)
    h00 = ham[0:1, 0:1].astype(F32)
    decay = di[0] + dk[...] + dl[...]
    out[0, 0] = real + (h00 * imag - term_k[:, 128:]) - decay * real
    out[1, 0] = imag - (h00 * real - term_k[:, :128]) - decay * imag


def base(me, pieces, ham, dk, dl, di):
    return call(
        base_body,
        shape((2, 16, 512, 128), F32),
        (16,),
        [pl.BlockSpec((2, 1, 128, 128), lambda t, me: (0, t, 0, 0))] * 4
        + [
            pl.BlockSpec((512, 512), lambda t, me: (0, 0)),
            pl.BlockSpec((512, 1), lambda t, me: (0, 0)),
            pl.BlockSpec((1, 128), lambda t, me: (0, 0)),
            pl.BlockSpec((1, 1, 1), lambda t, me: (t, 0, 0)),
        ],
        pl.BlockSpec((2, 1, 512, 128), lambda t, me: (0, t, 0, 0)),
        [pltpu.VMEM((512, 256), BF16)],
        1 << 31,
        12 << 20,
    )(me, *pieces, ham, dk, dl, di)


def project_body(me, la, w0, w1, w2, w3, z, rho, out, scr):
    @pl.when(pl.program_id(0) == 0)
    def _():
        for s, w in enumerate((w0, w1, w2, w3)):
            p = jnp.bitwise_xor(me[0], s)
            at = p // 2 * 512 + p % 2 * 128
            for c in range(2):
                scr[:, pl.ds(pl.multiple_of(at + c * 256, 128), 128)] = w[c]

    zr, zi = z[:, 0:1], z[:, 1:2]
    for n in range(4):
        cols = slice(n // 2 * 256, n // 2 * 256 + 256)
        x = jnp.dot(la[...], scr[:, n * 256 : n * 256 + 256], preferred_element_type=F32)
        rr, ri = rho[0:1, cols], rho[1:2, cols]
        x += zr * ri + zi * rr if n % 2 else zr * rr - zi * ri
        out[:, n * 256 : n * 256 + 256] = x.astype(out.dtype)


def project(me, la, pieces, z, rho, other, dtype):
    def at(t, me):
        half = me[0] % 2
        return ((1 - half if other else half) * 2 + t, 0)

    return call(
        project_body,
        shape((1024, 1024), dtype),
        (2,),
        [pl.BlockSpec((512, 2048), at)]
        + [whole((2, 2048, 128))] * 4
        + [pl.BlockSpec((512, 2), at), whole((2, 512))],
        pl.BlockSpec((512, 1024), lambda t, me: (t, 0)),
        [pltpu.VMEM((2048, 1024), BF16)],
        1 << 32,
        10 << 20,
    )(me, la, *pieces, z, rho)


def whole(dims):
    return pl.BlockSpec(dims, lambda t, me: (0,) * len(dims))


def second_body(far, me, lt, own, oth, w0, w1, w2, w3, ham, o0, o1, wcat, res):
    par = me[0] % 2
    lt_own = lt[:, pl.ds(pl.multiple_of(par * 1024, 128), 1024)]
    lt_oth = lt[:, pl.ds(pl.multiple_of((1 - par) * 1024, 128), 1024)]
    side = me[0] // 2
    side = pl.multiple_of((1 - side if far else side) * 256, 128)
    for c in range(2):
        for s, w in enumerate((w0, w1, w2, w3)):
            at = jnp.bitwise_xor(me[0], s) * 128
            wcat[:, pl.ds(pl.multiple_of(at + c * 512, 128), 128)] = w[c]
        cols = slice(c * 256, c * 256 + 256)
        y = jnp.dot(lt_own, own[:, cols], preferred_element_type=F32)
        y += jnp.dot(lt_oth, oth[:, cols], preferred_element_type=F32)
        y -= jnp.dot(wcat[:, c * 512 : c * 512 + 512], ham[:, pl.ds(side, 256)], preferred_element_type=F32)
        res[:, cols] = y.astype(BF16)
        for s, o in enumerate((o0, o1)):
            at = jnp.bitwise_xor(par, s) * 128 + c * 256
            o[c] = res[:, pl.ds(pl.multiple_of(at, 128), 128)]


def second(me, lt, own, oth, pieces, ham, far, first, steps):
    return call(
        functools.partial(second_body, far),
        (shape((2, steps * 512, 128)),) * 2,
        (steps,),
        [
            pl.BlockSpec((512, 2048), lambda t, me: (t + first, 0)),
            whole((1024, 512)),
            whole((1024, 512)),
        ]
        + [pl.BlockSpec((2, 512, 128), lambda t, me: (0, t + first, 0))] * 4
        + [whole((512, 512))],
        (pl.BlockSpec((2, 512, 128), lambda t, me: (0, t, 0)),) * 2,
        [pltpu.VMEM((512, 1024), BF16), pltpu.VMEM((512, 512), BF16)],
        1 << 31,
        8 << 20,
    )(me, lt, own, oth, *pieces, ham)


def mix_body(me, own, oth, ham, out_own, out_oth):
    low = me[1] == 0
    for j in range(4):
        halves = []
        for kc in (2 * j, 2 * j + 1):
            first = jnp.where(low, own[:, kc], oth[:, kc])
            last = jnp.where(low, oth[:, kc], own[:, kc])
            halves.append(jnp.stack([first, last], axis=1).reshape(512, 128))
        both = jnp.concatenate(halves, axis=1)
        y = jnp.dot(ham[...], both, preferred_element_type=F32).astype(BF16)
        for n, kc in enumerate((2 * j, 2 * j + 1)):
            part = y[:, n * 128 : n * 128 + 128].reshape(16, 2, 16, 128)
            out_own[:, kc] = jnp.where(low, part[:, 0], part[:, 1])
            out_oth[:, kc] = jnp.where(low, part[:, 1], part[:, 0])


def mix(me, own, oth, ham):
    block = pl.BlockSpec((16, 8, 16, 128), lambda t, me: (0, t, 0, 0))
    return call(
        mix_body,
        (shape((16, 32, 16, 128)),) * 2,
        (4,),
        [block, block, whole((512, 512))],
        (block, block),
        [],
        1 << 31,
        8 << 20,
    )(me, own, oth, ham)


def finish_body(me, b, t, v0, v1, v20, v21, v30, v31, *refs):
    out, v, first, scr = refs[-4:]
    for s, pieces in enumerate(((v0,), (v1,), (v20, v21), (v30, v31))):

        @pl.when(pl.program_id(0) == s)
        def _(pieces=pieces):
            first_row = 0
            for piece in pieces:
                v[:, first_row : first_row + piece.shape[1]] = piece[:, :, :, 0]
                first_row += piece.shape[1]

    @pl.loop(0, 4)
    def _(j):
        for c in range(2):
            for k in range(16):
                first[pl.ds((c * 16 + k) * 24, 16), :] = t[j, 2 * k + c].astype(F32)
        for i in range(16):
            real = b[0, i, j, 0] + v[1, i, j].astype(F32)
            imag = b[1, i, j, 0] - v[0, i, j].astype(F32)
            real += first[pl.ds(384 + i, 16, stride=24), :]
            imag -= first[pl.ds(i, 16, stride=24), :]
            scr[pl.ds(i * 40, 16, stride=2), :] = real
            scr[pl.ds(i * 40 + 1, 16, stride=2), :] = imag
        for i in range(16):
            out[i, j, 0] = scr[pl.ds(i * 40, 32), :].astype(BF16)


def finish(me, b, t, pieces, other, so_far):
    def side(s):
        return lambda t, me: (0, 0, jnp.bitwise_xor(me[0], t) if s else 0, side_of(me, other), 0, 0)

    def piece(v):
        return pl.BlockSpec((2, v.shape[1], 4, 1, 16, 128), side(0))

    views = [v.reshape(2, -1, 4, 2, 16, 128) for v in pieces]
    extra = [] if so_far is None else [so_far]
    return call(
        finish_body,
        shape((16, 16, 2, 32, 128)),
        (4,),
        [
            pl.BlockSpec((2, 16, 4, 1, 16, 128), side(1)),
            pl.BlockSpec((4, 32, 16, 128), lambda t, me: (jnp.bitwise_xor(me[0], t), 0, 0, 0)),
        ]
        + [piece(v) for v in views]
        + [pl.BlockSpec(memory_space=pl.ANY)] * len(extra),
        pl.BlockSpec(
            (16, 4, 1, 32, 128),
            lambda t, me: (0, jnp.bitwise_xor(me[0], t), side_of(me, other), 0, 0),
        ),
        [
            pltpu.VMEM((2, 16, 4, 16, 128), BF16),
            pltpu.VMEM((768, 128), F32),
            pltpu.VMEM((640, 128), F32),
        ],
        1 << 24,
        10 << 20,
        input_output_aliases={9: 0} if extra else {},
    )(me, b.reshape(2, 16, 16, 2, 16, 128), t, *views, *extra)


def swap(v, s):
    return lax.ppermute(v, ("zh", "c"), [(d, d ^ s) for d in range(4)])


def across(v, s):
    return lax.ppermute(v, ("zl", "zh"), [(d, d ^ s) for d in range(4)])


def to_owner(v, axes):
    return lax.all_to_all(v, axes, split_axis=0, concat_axis=0, tiled=True)


def per_device(g2, core_ham, dipole, field, rho, factors, damping):
    rows, width, _, _, cols = g2.shape
    plane = ("x", "y")
    pair_at = lax.axis_index(("x", "y", "zl"))
    idx_at = lax.axis_index(("zh", "c"))
    side = lax.axis_index("zl")
    me = jnp.stack([idx_at, side]).astype(jnp.int32)
    g = g2.reshape(rows, width * 2, cols)

    e2, e3 = pick(me, g, 2)
    w2, w3 = swap(e2, 2), swap(e3, 3)
    e0, e1 = pick(me, g, 0)
    w1 = swap(e1, 1)
    e = (e0, e1, e2, e3)
    w = [v.reshape(2, rows * 128, cols) for v in (e0, w1, w2, w3)]
    dealt_oth = deal(me, g, True)
    part_oth = to_owner(dealt_oth, plane)
    part_oth = lax.ppermute(part_oth, "zl", [(0, 1), (1, 0)])
    dealt_own = deal(me, g, False)
    part_own = to_owner(dealt_own, plane)

    hamil = 0.5 * (core_ham + core_ham.T) + field[0] * (0.5 * (dipole + dipole.T))
    ham = hamil.astype(BF16)
    rho_rows = lax.dynamic_slice_in_dim(rho, pair_at * rows, rows, 1)
    rho_local = lax.dynamic_slice_in_dim(rho_rows, idx_at * cols, cols, 2)
    z = lax.dot_general(
        factors, rho_local, (((1, 2), (1, 2)), ((), ())), preferred_element_type=F32
    )
    slab = rho[:, 0, :].astype(F32)
    la = flat(me, factors)
    di = lax.dynamic_slice_in_dim(damping, pair_at * rows, rows, 0) + damping[0]
    dl = lax.dynamic_slice_in_dim(damping, idx_at * cols, cols, 0).reshape(1, cols)
    b = base(me, e, ham, damping.reshape(width, 1), dl, di.reshape(rows, 1, 1))
    lt = turn(me, la)

    theirs = project(me, la, w, z, slab, True, BF16)
    theirs = swap(theirs, 1)
    mine = project(me, la, w, z, slab, False, F32)
    share = (mine + theirs.astype(F32)).astype(BF16).reshape(16, 64, 1024)
    share = to_owner(share, plane)
    share = jnp.sum(share.astype(F32), axis=0).astype(BF16)
    shares = [share] + [across(share, s) for s in (1, 2, 3)]
    aux = sum(v.astype(F32) for v in shares).astype(BF16)

    half = lax.axis_index("zh")
    far = lax.dynamic_slice_in_dim(aux, (1 - half) * 512, 512, 1)
    near = lax.dynamic_slice_in_dim(aux, half * 512, 512, 1)
    far = to_owner(jnp.broadcast_to(far[None], (16, 64, 512)), plane).reshape(1024, 512)
    far_oth = swap(far, 1)
    near = to_owner(jnp.broadcast_to(near[None], (16, 64, 512)), plane).reshape(1024, 512)
    near_oth = swap(near, 1)

    mixed_own, mixed_oth = mix(me, part_own, part_oth, ham)
    mixed_oth = lax.ppermute(mixed_oth, "zl", [(0, 1), (1, 0)])
    term_own = to_owner(mixed_own, plane)
    term_oth = to_owner(mixed_oth, plane)

    out_far = []
    for h in range(2):
        r2, r3 = second(me, lt, far, far_oth, w, ham, True, h, 1 + 2 * h)
        out_far.append((swap(r2, 2), swap(r3, 3)))
    r0, r1 = second(me, lt, near, near_oth, w, ham, False, 0, 4)
    r1 = swap(r1, 1)
    pieces = [r0, r1, *[out_far[h][s] for s in range(2) for h in range(2)]]
    out = finish(me, b, term_own, pieces, False, None)
    out = finish(me, b, term_oth, pieces, True, out)
    return out.reshape(rows, width, 2, 1, cols)


def solution(mesh):
    fine = Mesh(mesh.devices.reshape(4, 4, 2, 2, 2), ("x", "y", "zl", "zh", "c"))
    pair, idx = ("x", "y", "zl"), ("zh", "c")
    placed = (P(pair, None, None, None, idx), P(), P(), P(), P(), P(None, pair, idx), P())
    return jax.shard_map(
        per_device,
        mesh=fine,
        in_specs=placed,
        out_specs=P(pair, None, None, None, idx),
        check_vma=False,
    )
```

```python
import functools

import jax
import jax.numpy as jnp
from jax import lax
from jax.experimental import pallas as pl
from jax.experimental.pallas import tpu as pltpu
from jax.sharding import Mesh, PartitionSpec as P

F32 = jnp.float32
BF16 = jnp.bfloat16


def shape(dims, dtype=BF16):
    return jax.ShapeDtypeStruct(dims, dtype)


def call(body, out, grid, ins, outs, scratch, flops, moved, prefetch=1, **kw):
    return pl.pallas_call(
        body,
        out_shape=out,
        grid_spec=pltpu.PrefetchScalarGridSpec(
            num_scalar_prefetch=prefetch,
            grid=grid,
            in_specs=ins,
            out_specs=outs,
            scratch_shapes=scratch,
        ),
        compiler_params=pltpu.CompilerParams(
            dimension_semantics=("arbitrary",) * len(grid), vmem_limit_bytes=56 << 20
        ),
        cost_estimate=pl.CostEstimate(flops=flops, bytes_accessed=moved, transcendentals=0),
        **kw,
    )


def hold(step, first, count):
    return jnp.clip(step - first, 0, count - 1)


def pick_body(me, g, e0, e1, scr):
    step = pl.program_id(0)
    for sub in range(4):
        for i in range(16):
            scr[pl.ds(i * 40, 32), :] = g[i, sub * 32 : sub * 32 + 32, :].astype(F32)
        for s, e in enumerate((e0, e1)):

            @pl.when(step // 2 == s)
            def _(e=e, sub=sub):
                for c in range(2):
                    for i in range(16):
                        rows = scr[pl.ds(i * 40 + c, 16, stride=2), :]
                        e[c, i, sub * 16 : sub * 16 + 16, :] = rows.astype(BF16)


def pick(me, g, first):
    def where(t, me):
        return jnp.bitwise_xor(me[0], first + t // 2) * 2 + t % 2

    piece = lambda s: pl.BlockSpec((2, 16, 64, 128), lambda t, me: (0, 0, hold(t, 2 * s, 2), 0))
    return call(
        pick_body,
        (shape((2, 16, 128, 128)),) * 2,
        (4,),
        [pl.BlockSpec((16, 128, 128), lambda t, me: (0, where(t, me), 0))],
        (piece(0), piece(1)),
        [pltpu.VMEM((640, 128), F32)],
        1 << 24,
        4 << 20,
    )(me, g)


def deal_body(me, g, t_out, scr):
    for sub in range(4):
        for i in range(16):
            scr[pl.ds(i * 40, 32), :] = g[i, sub * 32 : sub * 32 + 32, :].astype(F32)
        for kc in range(32):
            t_out[sub, kc] = scr[pl.ds(kc, 16, stride=40), :].astype(BF16)


def side_of(me, other):
    return 1 - me[1] if other else me[1]


def deal(me, g):
    return call(
        deal_body,
        shape((32, 32, 16, 128)),
        (8,),
        [pl.BlockSpec((16, 128, 128), lambda t, me: (0, t, 0))],
        pl.BlockSpec((4, 32, 16, 128), lambda t, me: (t, 0, 0, 0)),
        [pltpu.VMEM((640, 128), F32)],
        1 << 24,
        8 << 20,
    )(me, g)


def flat_body(me, l, la, scr):
    for q in range(128):
        scr[pl.ds(q * 24, 16), :] = l[q].astype(F32)
    for m in range(16):
        rows = scr[pl.ds(m, 128, stride=24), :]
        la[:, m * 128 : m * 128 + 128] = rows.astype(BF16)


def flat(me, factors):
    return call(
        flat_body,
        shape((2048, 2048)),
        (16,),
        [pl.BlockSpec((128, 16, 128), lambda t, me: (t, 0, 0))],
        pl.BlockSpec((128, 2048), lambda t, me: (t, 0)),
        [pltpu.VMEM((3072, 128), F32)],
        1 << 24,
        16 << 20,
    )(me, factors)


def turn_body(me, la, lt):
    for m in range(8):
        lt[m * 128 : m * 128 + 128, :] = la[:, m * 128 : m * 128 + 128].T


def turn(me, la):
    return call(
        turn_body,
        shape((2048, 2048)),
        (2, 8),
        [pl.BlockSpec((256, 1024), lambda r, t, me: (t, r))],
        pl.BlockSpec((1024, 256), lambda r, t, me: (r, t)),
        [],
        1 << 26,
        16 << 20,
    )(me, la)


def base_body(me, e0, e1, e2, e3, ham, dk, dl, di, out, scr):
    for s, e in enumerate((e0, e1, e2, e3)):
        at = pl.multiple_of(jnp.bitwise_xor(me[0], s) * 128, 128)
        for c in range(2):
            scr[pl.ds(at, 128), c * 128 : c * 128 + 128] = e[c, 0]
    term_k = jnp.dot(ham[...], scr[...], preferred_element_type=F32)
    real = scr[:, :128].astype(F32)
    imag = scr[:, 128:].astype(F32)
    h00 = ham[0:1, 0:1].astype(F32)
    decay = di[0] + dk[...] + dl[...]
    out[0, 0] = real + (h00 * imag - term_k[:, 128:]) - decay * real
    out[1, 0] = imag - (h00 * real - term_k[:, :128]) - decay * imag


def base(me, pieces, ham, dk, dl, di):
    return call(
        base_body,
        shape((2, 16, 512, 128), F32),
        (16,),
        [pl.BlockSpec((2, 1, 128, 128), lambda t, me: (0, t, 0, 0))] * 4
        + [
            pl.BlockSpec((512, 512), lambda t, me: (0, 0)),
            pl.BlockSpec((512, 1), lambda t, me: (0, 0)),
            pl.BlockSpec((1, 128), lambda t, me: (0, 0)),
            pl.BlockSpec((1, 1, 1), lambda t, me: (t, 0, 0)),
        ],
        pl.BlockSpec((2, 1, 512, 128), lambda t, me: (0, t, 0, 0)),
        [pltpu.VMEM((512, 256), BF16)],
        1 << 31,
        12 << 20,
    )(me, *pieces, ham, dk, dl, di)


def project_body(me, la, w0, w1, w2, w3, z, rho, out, scr):
    @pl.when(pl.program_id(0) == 0)
    def _():
        for s, w in enumerate((w0, w1, w2, w3)):
            p = jnp.bitwise_xor(me[0], s)
            at = p // 2 * 512 + p % 2 * 128
            for c in range(2):
                scr[:, pl.ds(pl.multiple_of(at + c * 256, 128), 128)] = w[c]

    zr, zi = z[:, 0:1], z[:, 1:2]
    for n in range(4):
        cols = slice(n // 2 * 256, n // 2 * 256 + 256)
        x = jnp.dot(la[...], scr[:, n * 256 : n * 256 + 256], preferred_element_type=F32)
        rr, ri = rho[0:1, cols], rho[1:2, cols]
        x += zr * ri + zi * rr if n % 2 else zr * rr - zi * ri
        out[:, n * 256 : n * 256 + 256] = x.astype(out.dtype)


def project(me, la, pieces, z, rho, other, dtype):
    def at(t, me):
        half = me[0] % 2
        return ((1 - half if other else half) * 2 + t, 0)

    return call(
        project_body,
        shape((1024, 1024), dtype),
        (2,),
        [pl.BlockSpec((512, 2048), at)]
        + [whole((2, 2048, 128))] * 4
        + [pl.BlockSpec((512, 2), at), whole((2, 512))],
        pl.BlockSpec((512, 1024), lambda t, me: (t, 0)),
        [pltpu.VMEM((2048, 1024), BF16)],
        1 << 32,
        10 << 20,
    )(me, la, *pieces, z, rho)


def whole(dims):
    return pl.BlockSpec(dims, lambda t, me: (0,) * len(dims))


def second_body(far, me, lt, own, oth, w0, w1, w2, w3, ham, o0, o1, wcat, res):
    par = me[0] % 2
    lt_own = lt[:, pl.ds(pl.multiple_of(par * 1024, 128), 1024)]
    lt_oth = lt[:, pl.ds(pl.multiple_of((1 - par) * 1024, 128), 1024)]
    side = me[0] // 2
    side = pl.multiple_of((1 - side if far else side) * 256, 128)
    for c in range(2):
        for s, w in enumerate((w0, w1, w2, w3)):
            at = jnp.bitwise_xor(me[0], s) * 128
            wcat[:, pl.ds(pl.multiple_of(at + c * 512, 128), 128)] = w[c]
        cols = slice(c * 256, c * 256 + 256)
        y = jnp.dot(lt_own, own[:, cols], preferred_element_type=F32)
        y += jnp.dot(lt_oth, oth[:, cols], preferred_element_type=F32)
        y -= jnp.dot(wcat[:, c * 512 : c * 512 + 512], ham[:, pl.ds(side, 256)], preferred_element_type=F32)
        res[:, cols] = y.astype(BF16)
        for s, o in enumerate((o0, o1)):
            at = jnp.bitwise_xor(par, s) * 128 + c * 256
            o[c] = res[:, pl.ds(pl.multiple_of(at, 128), 128)]


def second(me, lt, own, oth, pieces, ham, far, first, steps):
    return call(
        functools.partial(second_body, far),
        (shape((2, steps * 512, 128)),) * 2,
        (steps,),
        [
            pl.BlockSpec((512, 2048), lambda t, me: (t + first, 0)),
            whole((1024, 512)),
            whole((1024, 512)),
        ]
        + [pl.BlockSpec((2, 512, 128), lambda t, me: (0, t + first, 0))] * 4
        + [whole((512, 512))],
        (pl.BlockSpec((2, 512, 128), lambda t, me: (0, t, 0)),) * 2,
        [pltpu.VMEM((512, 1024), BF16), pltpu.VMEM((512, 512), BF16)],
        1 << 31,
        8 << 20,
    )(me, lt, own, oth, *pieces, ham)


def mix_body(me, own, oth, ham, out_own, out_oth):
    low = me[1] == 0
    for j in range(4):
        halves = []
        for kc in (2 * j, 2 * j + 1):
            first = jnp.where(low, own[:, 0, kc], oth[:, kc])
            last = jnp.where(low, oth[:, kc], own[:, 0, kc])
            halves.append(jnp.stack([first, last], axis=1).reshape(512, 128))
        both = jnp.concatenate(halves, axis=1)
        y = jnp.dot(ham[...], both, preferred_element_type=F32).astype(BF16)
        for n, kc in enumerate((2 * j, 2 * j + 1)):
            part = y[:, n * 128 : n * 128 + 128].reshape(16, 2, 16, 128)
            out_own[:, kc] = jnp.where(low, part[:, 0], part[:, 1])
            out_oth[:, kc] = jnp.where(low, part[:, 1], part[:, 0])


def mix(me, own, oth, ham):
    block = pl.BlockSpec((16, 8, 16, 128), lambda t, me: (0, t, 0, 0))
    return call(
        mix_body,
        (shape((16, 32, 16, 128)),) * 2,
        (4,),
        [
            pl.BlockSpec((16, 1, 8, 16, 128), lambda t, me: (0, me[1], t, 0, 0)),
            block,
            whole((512, 512)),
        ],
        (block, block),
        [],
        1 << 31,
        8 << 20,
    )(me, own, oth, ham)


def finish_body(me, b, t, v0, v1, v20, v21, v30, v31, *refs):
    out, v, first, scr = refs[-4:]
    for s, pieces in enumerate(((v0,), (v1,), (v20, v21), (v30, v31))):

        @pl.when(pl.program_id(0) == s)
        def _(pieces=pieces):
            first_row = 0
            for piece in pieces:
                v[:, first_row : first_row + piece.shape[1]] = piece[:, :, :, 0]
                first_row += piece.shape[1]

    @pl.loop(0, 4)
    def _(j):
        for c in range(2):
            for k in range(16):
                first[pl.ds((c * 16 + k) * 24, 16), :] = t[j, 2 * k + c].astype(F32)
        for i in range(16):
            real = b[0, i, j, 0] + v[1, i, j].astype(F32)
            imag = b[1, i, j, 0] - v[0, i, j].astype(F32)
            real += first[pl.ds(384 + i, 16, stride=24), :]
            imag -= first[pl.ds(i, 16, stride=24), :]
            scr[pl.ds(i * 40, 16, stride=2), :] = real
            scr[pl.ds(i * 40 + 1, 16, stride=2), :] = imag
        for i in range(16):
            out[i, j, 0] = scr[pl.ds(i * 40, 32), :].astype(BF16)


def finish(me, b, t, pieces, other, so_far):
    def side(s):
        return lambda t, me: (0, 0, jnp.bitwise_xor(me[0], t) if s else 0, side_of(me, other), 0, 0)

    def piece(v):
        return pl.BlockSpec((2, v.shape[1], 4, 1, 16, 128), side(0))

    views = [v.reshape(2, -1, 4, 2, 16, 128) for v in pieces]
    extra = [] if so_far is None else [so_far]
    return call(
        finish_body,
        shape((16, 16, 2, 32, 128)),
        (4,),
        [
            pl.BlockSpec((2, 16, 4, 1, 16, 128), side(1)),
            pl.BlockSpec((4, 32, 16, 128), lambda t, me: (jnp.bitwise_xor(me[0], t), 0, 0, 0)),
        ]
        + [piece(v) for v in views]
        + [pl.BlockSpec(memory_space=pl.ANY)] * len(extra),
        pl.BlockSpec(
            (16, 4, 1, 32, 128),
            lambda t, me: (0, jnp.bitwise_xor(me[0], t), side_of(me, other), 0, 0),
        ),
        [
            pltpu.VMEM((2, 16, 4, 16, 128), BF16),
            pltpu.VMEM((768, 128), F32),
            pltpu.VMEM((640, 128), F32),
        ],
        1 << 24,
        10 << 20,
        input_output_aliases={9: 0} if extra else {},
    )(me, b.reshape(2, 16, 16, 2, 16, 128), t, *views, *extra)


def swap(v, s):
    return lax.ppermute(v, ("zh", "c"), [(d, d ^ s) for d in range(4)])


def across(v, s):
    return lax.ppermute(v, ("zl", "zh"), [(d, d ^ s) for d in range(4)])


def to_owner(v, axes):
    return lax.all_to_all(v, axes, split_axis=0, concat_axis=0, tiled=True)


def per_device(g2, core_ham, dipole, field, rho, factors, damping):
    rows, width, _, _, cols = g2.shape
    plane = ("x", "y")
    pair_at = lax.axis_index(("x", "y", "zl"))
    idx_at = lax.axis_index(("zh", "c"))
    side = lax.axis_index("zl")
    me = jnp.stack([idx_at, side]).astype(jnp.int32)
    g = g2.reshape(rows, width * 2, cols)

    e2, e3 = pick(me, g, 2)
    w2, w3 = swap(e2, 2), swap(e3, 3)
    e0, e1 = pick(me, g, 0)
    w1 = swap(e1, 1)
    e = (e0, e1, e2, e3)
    w = [v.reshape(2, rows * 128, cols) for v in (e0, w1, w2, w3)]
    dealt = deal(me, g)
    part = to_owner(dealt, plane).reshape(16, 2, 32, 16, 128)
    part_oth = lax.dynamic_index_in_dim(part, 1 - side, 1, keepdims=False)
    part_oth = lax.ppermute(part_oth, "zl", [(0, 1), (1, 0)])

    hamil = 0.5 * (core_ham + core_ham.T) + field[0] * (0.5 * (dipole + dipole.T))
    ham = hamil.astype(BF16)
    rho_rows = lax.dynamic_slice_in_dim(rho, pair_at * rows, rows, 1)
    rho_local = lax.dynamic_slice_in_dim(rho_rows, idx_at * cols, cols, 2)
    z = lax.dot_general(
        factors, rho_local, (((1, 2), (1, 2)), ((), ())), preferred_element_type=F32
    )
    slab = rho[:, 0, :].astype(F32)
    la = flat(me, factors)
    di = lax.dynamic_slice_in_dim(damping, pair_at * rows, rows, 0) + damping[0]
    dl = lax.dynamic_slice_in_dim(damping, idx_at * cols, cols, 0).reshape(1, cols)
    b = base(me, e, ham, damping.reshape(width, 1), dl, di.reshape(rows, 1, 1))
    lt = turn(me, la)

    theirs = project(me, la, w, z, slab, True, BF16)
    theirs = swap(theirs, 1)
    mine = project(me, la, w, z, slab, False, F32)
    share = (mine + theirs.astype(F32)).astype(BF16).reshape(16, 64, 1024)
    share = to_owner(share, plane)
    share = jnp.sum(share.astype(F32), axis=0).astype(BF16)
    shares = [share] + [across(share, s) for s in (1, 2, 3)]
    aux = sum(v.astype(F32) for v in shares).astype(BF16)

    half = lax.axis_index("zh")
    far = lax.dynamic_slice_in_dim(aux, (1 - half) * 512, 512, 1)
    near = lax.dynamic_slice_in_dim(aux, half * 512, 512, 1)
    far = to_owner(jnp.broadcast_to(far[None], (16, 64, 512)), plane).reshape(1024, 512)
    far_oth = swap(far, 1)
    near = to_owner(jnp.broadcast_to(near[None], (16, 64, 512)), plane).reshape(1024, 512)
    near_oth = swap(near, 1)

    mixed_own, mixed_oth = mix(me, part, part_oth, ham)
    mixed_oth = lax.ppermute(mixed_oth, "zl", [(0, 1), (1, 0)])
    term_own = to_owner(mixed_own, plane)
    term_oth = to_owner(mixed_oth, plane)

    out_far = []
    for h in range(2):
        r2, r3 = second(me, lt, far, far_oth, w, ham, True, h, 1 + 2 * h)
        out_far.append((swap(r2, 2), swap(r3, 3)))
    r0, r1 = second(me, lt, near, near_oth, w, ham, False, 0, 4)
    r1 = swap(r1, 1)
    pieces = [r0, r1, *[out_far[h][s] for s in range(2) for h in range(2)]]
    out = finish(me, b, term_own, pieces, False, None)
    out = finish(me, b, term_oth, pieces, True, out)
    return out.reshape(rows, width, 2, 1, cols)


def solution(mesh):
    fine = Mesh(mesh.devices.reshape(4, 4, 2, 2, 2), ("x", "y", "zl", "zh", "c"))
    pair, idx = ("x", "y", "zl"), ("zh", "c")
    placed = (P(pair, None, None, None, idx), P(), P(), P(), P(), P(None, pair, idx), P())
    return jax.shard_map(
        per_device,
        mesh=fine,
        in_specs=placed,
        out_specs=P(pair, None, None, None, idx),
        check_vma=False,
    )
```

```python
import functools

import jax
import jax.numpy as jnp
from jax import lax
from jax.experimental import pallas as pl
from jax.experimental.pallas import tpu as pltpu
from jax.sharding import Mesh, PartitionSpec as P

F32 = jnp.float32
BF16 = jnp.bfloat16


def shape(dims, dtype=BF16):
    return jax.ShapeDtypeStruct(dims, dtype)


def call(body, out, grid, ins, outs, scratch, flops, moved, prefetch=1, **kw):
    return pl.pallas_call(
        body,
        out_shape=out,
        grid_spec=pltpu.PrefetchScalarGridSpec(
            num_scalar_prefetch=prefetch,
            grid=grid,
            in_specs=ins,
            out_specs=outs,
            scratch_shapes=scratch,
        ),
        compiler_params=pltpu.CompilerParams(
            dimension_semantics=("arbitrary",) * len(grid), vmem_limit_bytes=56 << 20
        ),
        cost_estimate=pl.CostEstimate(flops=flops, bytes_accessed=moved, transcendentals=0),
        **kw,
    )


def hold(step, first, count):
    return jnp.clip(step - first, 0, count - 1)


def pick_body(me, g, e0, e1, scr):
    step = pl.program_id(0)
    for sub in range(4):
        for i in range(16):
            scr[pl.ds(i * 40, 32), :] = g[i, sub * 32 : sub * 32 + 32, :].astype(F32)
        for s, e in enumerate((e0, e1)):

            @pl.when(step // 2 == s)
            def _(e=e, sub=sub):
                for c in range(2):
                    for i in range(16):
                        rows = scr[pl.ds(i * 40 + c, 16, stride=2), :]
                        e[c, i, sub * 16 : sub * 16 + 16, :] = rows.astype(BF16)


def pick(me, g, first):
    def where(t, me):
        return jnp.bitwise_xor(me[0], first + t // 2) * 2 + t % 2

    piece = lambda s: pl.BlockSpec((2, 16, 64, 128), lambda t, me: (0, 0, hold(t, 2 * s, 2), 0))
    return call(
        pick_body,
        (shape((2, 16, 128, 128)),) * 2,
        (4,),
        [pl.BlockSpec((16, 128, 128), lambda t, me: (0, where(t, me), 0))],
        (piece(0), piece(1)),
        [pltpu.VMEM((640, 128), F32)],
        1 << 24,
        4 << 20,
    )(me, g)


def deal_body(me, *refs):
    gs, t_out, scr = refs[:4], refs[4], refs[5]
    for sub, g in enumerate(gs):
        for i in range(16):
            scr[pl.ds(i * 40, 32), :] = g[i].astype(F32)
        for kc in range(32):
            t_out[sub, kc] = scr[pl.ds(kc, 16, stride=40), :].astype(BF16)


def side_of(me, other):
    return 1 - me[1] if other else me[1]


def deal(me, g, other):
    def piece(sub):
        at = lambda t, me: (0, (t * 4 + sub) * 2 + side_of(me, other), 0)
        return pl.BlockSpec((16, 32, 128), at)

    return call(
        deal_body,
        shape((16, 32, 16, 128)),
        (4,),
        [piece(sub) for sub in range(4)],
        pl.BlockSpec((4, 32, 16, 128), lambda t, me: (t, 0, 0, 0)),
        [pltpu.VMEM((640, 128), F32)],
        1 << 24,
        4 << 20,
    )(me, g, g, g, g)


def flat_body(me, l, la, scr):
    for q in range(128):
        scr[pl.ds(q * 24, 16), :] = l[q].astype(F32)
    for m in range(16):
        rows = scr[pl.ds(m, 128, stride=24), :]
        la[:, m * 128 : m * 128 + 128] = rows.astype(BF16)


def flat(me, factors):
    return call(
        flat_body,
        shape((2048, 2048)),
        (16,),
        [pl.BlockSpec((128, 16, 128), lambda t, me: (t, 0, 0))],
        pl.BlockSpec((128, 2048), lambda t, me: (t, 0)),
        [pltpu.VMEM((3072, 128), F32)],
        1 << 24,
        16 << 20,
    )(me, factors)


def turn_body(me, la, lt):
    for m in range(8):
        lt[m * 128 : m * 128 + 128, :] = la[:, m * 128 : m * 128 + 128].T


def turn(me, la):
    return call(
        turn_body,
        shape((2048, 2048)),
        (2, 8),
        [pl.BlockSpec((256, 1024), lambda r, t, me: (t, r))],
        pl.BlockSpec((1024, 256), lambda r, t, me: (r, t)),
        [],
        1 << 26,
        16 << 20,
    )(me, la)


def base_body(me, e0, e1, e2, e3, ham, dk, dl, di, out, scr):
    for s, e in enumerate((e0, e1, e2, e3)):
        at = pl.multiple_of(jnp.bitwise_xor(me[0], s) * 128, 128)
        for c in range(2):
            scr[pl.ds(at, 128), c * 128 : c * 128 + 128] = e[c, 0]
    term_k = jnp.dot(ham[...], scr[...], preferred_element_type=F32)
    real = scr[:, :128].astype(F32)
    imag = scr[:, 128:].astype(F32)
    h00 = ham[0:1, 0:1].astype(F32)
    decay = di[0] + dk[...] + dl[...]
    out[0, 0] = real + (h00 * imag - term_k[:, 128:]) - decay * real
    out[1, 0] = imag - (h00 * real - term_k[:, :128]) - decay * imag


def base(me, pieces, ham, dk, dl, di):
    return call(
        base_body,
        shape((2, 16, 512, 128), F32),
        (16,),
        [pl.BlockSpec((2, 1, 128, 128), lambda t, me: (0, t, 0, 0))] * 4
        + [
            pl.BlockSpec((512, 512), lambda t, me: (0, 0)),
            pl.BlockSpec((512, 1), lambda t, me: (0, 0)),
            pl.BlockSpec((1, 128), lambda t, me: (0, 0)),
            pl.BlockSpec((1, 1, 1), lambda t, me: (t, 0, 0)),
        ],
        pl.BlockSpec((2, 1, 512, 128), lambda t, me: (0, t, 0, 0)),
        [pltpu.VMEM((512, 256), BF16)],
        1 << 31,
        12 << 20,
    )(me, *pieces, ham, dk, dl, di)


def project_body(me, la, w0, w1, w2, w3, z, rho, out, scr):
    @pl.when(pl.program_id(0) == 0)
    def _():
        for s, w in enumerate((w0, w1, w2, w3)):
            p = jnp.bitwise_xor(me[0], s)
            at = p // 2 * 512 + p % 2 * 128
            for c in range(2):
                scr[:, pl.ds(pl.multiple_of(at + c * 256, 128), 128)] = w[c]

    zr, zi = z[:, 0:1], z[:, 1:2]
    for n in range(4):
        cols = slice(n // 2 * 256, n // 2 * 256 + 256)
        x = jnp.dot(la[...], scr[:, n * 256 : n * 256 + 256], preferred_element_type=F32)
        rr, ri = rho[0:1, cols], rho[1:2, cols]
        x += zr * ri + zi * rr if n % 2 else zr * rr - zi * ri
        out[:, n * 256 : n * 256 + 256] = x.astype(out.dtype)


def project(me, la, pieces, z, rho, other, dtype):
    def at(t, me):
        half = me[0] % 2
        return ((1 - half if other else half) * 2 + t, 0)

    return call(
        project_body,
        shape((1024, 1024), dtype),
        (2,),
        [pl.BlockSpec((512, 2048), at)]
        + [whole((2, 2048, 128))] * 4
        + [pl.BlockSpec((512, 2), at), whole((2, 512))],
        pl.BlockSpec((512, 1024), lambda t, me: (t, 0)),
        [pltpu.VMEM((2048, 1024), BF16)],
        1 << 32,
        10 << 20,
    )(me, la, *pieces, z, rho)


def whole(dims):
    return pl.BlockSpec(dims, lambda t, me: (0,) * len(dims))


def second_body(far, me, lt, own, oth, w0, w1, w2, w3, ham, o0, o1, wcat, res):
    par = me[0] % 2
    lt_own = lt[:, pl.ds(pl.multiple_of(par * 1024, 128), 1024)]
    lt_oth = lt[:, pl.ds(pl.multiple_of((1 - par) * 1024, 128), 1024)]
    side = me[0] // 2
    side = pl.multiple_of((1 - side if far else side) * 256, 128)
    for c in range(2):
        for s, w in enumerate((w0, w1, w2, w3)):
            at = jnp.bitwise_xor(me[0], s) * 128
            wcat[:, pl.ds(pl.multiple_of(at + c * 512, 128), 128)] = w[c]
        cols = slice(c * 256, c * 256 + 256)
        y = jnp.dot(lt_own, own[:, cols], preferred_element_type=F32)
        y += jnp.dot(lt_oth, oth[:, cols], preferred_element_type=F32)
        y -= jnp.dot(wcat[:, c * 512 : c * 512 + 512], ham[:, pl.ds(side, 256)], preferred_element_type=F32)
        res[:, cols] = y.astype(BF16)
        for s, o in enumerate((o0, o1)):
            at = jnp.bitwise_xor(par, s) * 128 + c * 256
            o[c] = res[:, pl.ds(pl.multiple_of(at, 128), 128)]


def second(me, lt, own, oth, pieces, ham, far, first, steps):
    def which(t, me):
        return (0, 1 - me[0] // 2 if far else me[0] // 2)

    return call(
        functools.partial(second_body, far),
        (shape((2, steps * 512, 128)),) * 2,
        (steps,),
        [
            pl.BlockSpec((512, 2048), lambda t, me: (t + first, 0)),
            pl.BlockSpec((1024, 512), which),
            pl.BlockSpec((1024, 512), which),
        ]
        + [pl.BlockSpec((2, 512, 128), lambda t, me: (0, t + first, 0))] * 4
        + [whole((512, 512))],
        (pl.BlockSpec((2, 512, 128), lambda t, me: (0, t, 0)),) * 2,
        [pltpu.VMEM((512, 1024), BF16), pltpu.VMEM((512, 512), BF16)],
        1 << 31,
        8 << 20,
    )(me, lt, own, oth, *pieces, ham)


def mix_body(me, own, oth, ham, out_own, out_oth):
    low = me[1] == 0
    for j in range(4):
        halves = []
        for kc in (2 * j, 2 * j + 1):
            first = jnp.where(low, own[:, kc], oth[:, kc])
            last = jnp.where(low, oth[:, kc], own[:, kc])
            halves.append(jnp.stack([first, last], axis=1).reshape(512, 128))
        both = jnp.concatenate(halves, axis=1)
        y = jnp.dot(ham[...], both, preferred_element_type=F32).astype(BF16)
        for n, kc in enumerate((2 * j, 2 * j + 1)):
            part = y[:, n * 128 : n * 128 + 128].reshape(16, 2, 16, 128)
            out_own[:, kc] = jnp.where(low, part[:, 0], part[:, 1])
            out_oth[:, kc] = jnp.where(low, part[:, 1], part[:, 0])


def mix(me, own, oth, ham):
    block = pl.BlockSpec((16, 8, 16, 128), lambda t, me: (0, t, 0, 0))
    return call(
        mix_body,
        (shape((16, 32, 16, 128)),) * 2,
        (4,),
        [block, block, whole((512, 512))],
        (block, block),
        [],
        1 << 31,
        8 << 20,
    )(me, own, oth, ham)


def finish_body(me, b, t, v0, v1, v20, v21, v30, v31, *refs):
    out, v, first, scr = refs[-4:]
    for s, pieces in enumerate(((v0,), (v1,), (v20, v21), (v30, v31))):

        @pl.when(pl.program_id(0) == s)
        def _(pieces=pieces):
            first_row = 0
            for piece in pieces:
                v[:, first_row : first_row + piece.shape[1]] = piece[:, :, :, 0]
                first_row += piece.shape[1]

    @pl.loop(0, 4)
    def _(j):
        for c in range(2):
            for k in range(16):
                first[pl.ds((c * 16 + k) * 24, 16), :] = t[j, 2 * k + c].astype(F32)
        for i in range(16):
            real = b[0, i, j, 0] + v[1, i, j].astype(F32)
            imag = b[1, i, j, 0] - v[0, i, j].astype(F32)
            real += first[pl.ds(384 + i, 16, stride=24), :]
            imag -= first[pl.ds(i, 16, stride=24), :]
            scr[pl.ds(i * 40, 16, stride=2), :] = real
            scr[pl.ds(i * 40 + 1, 16, stride=2), :] = imag
        for i in range(16):
            out[i, j, 0] = scr[pl.ds(i * 40, 32), :].astype(BF16)


def finish(me, b, t, pieces, other, so_far):
    def side(s):
        return lambda t, me: (0, 0, jnp.bitwise_xor(me[0], t) if s else 0, side_of(me, other), 0, 0)

    def piece(v):
        return pl.BlockSpec((2, v.shape[1], 4, 1, 16, 128), side(0))

    views = [v.reshape(2, -1, 4, 2, 16, 128) for v in pieces]
    extra = [] if so_far is None else [so_far]
    return call(
        finish_body,
        shape((16, 16, 2, 32, 128)),
        (4,),
        [
            pl.BlockSpec((2, 16, 4, 1, 16, 128), side(1)),
            pl.BlockSpec((4, 32, 16, 128), lambda t, me: (jnp.bitwise_xor(me[0], t), 0, 0, 0)),
        ]
        + [piece(v) for v in views]
        + [pl.BlockSpec(memory_space=pl.ANY)] * len(extra),
        pl.BlockSpec(
            (16, 4, 1, 32, 128),
            lambda t, me: (0, jnp.bitwise_xor(me[0], t), side_of(me, other), 0, 0),
        ),
        [
            pltpu.VMEM((2, 16, 4, 16, 128), BF16),
            pltpu.VMEM((768, 128), F32),
            pltpu.VMEM((640, 128), F32),
        ],
        1 << 24,
        10 << 20,
        input_output_aliases={9: 0} if extra else {},
    )(me, b.reshape(2, 16, 16, 2, 16, 128), t, *views, *extra)


def swap(v, s):
    return lax.ppermute(v, ("zh", "c"), [(d, d ^ s) for d in range(4)])


def across(v, s):
    return lax.ppermute(v, ("zl", "zh"), [(d, d ^ s) for d in range(4)])


def to_owner(v, axes):
    return lax.all_to_all(v, axes, split_axis=0, concat_axis=0, tiled=True)


def per_device(g2, core_ham, dipole, field, rho, factors, damping):
    rows, width, _, _, cols = g2.shape
    plane = ("x", "y")
    pair_at = lax.axis_index(("x", "y", "zl"))
    idx_at = lax.axis_index(("zh", "c"))
    side = lax.axis_index("zl")
    me = jnp.stack([idx_at, side]).astype(jnp.int32)
    g = g2.reshape(rows, width * 2, cols)

    e2, e3 = pick(me, g, 2)
    w2, w3 = swap(e2, 2), swap(e3, 3)
    e0, e1 = pick(me, g, 0)
    w1 = swap(e1, 1)
    e = (e0, e1, e2, e3)
    w = [v.reshape(2, rows * 128, cols) for v in (e0, w1, w2, w3)]
    dealt_oth = deal(me, g, True)
    part_oth = to_owner(dealt_oth, plane)
    part_oth = lax.ppermute(part_oth, "zl", [(0, 1), (1, 0)])
    dealt_own = deal(me, g, False)
    part_own = to_owner(dealt_own, plane)

    hamil = 0.5 * (core_ham + core_ham.T) + field[0] * (0.5 * (dipole + dipole.T))
    ham = hamil.astype(BF16)
    rho_rows = lax.dynamic_slice_in_dim(rho, pair_at * rows, rows, 1)
    rho_local = lax.dynamic_slice_in_dim(rho_rows, idx_at * cols, cols, 2)
    z = lax.dot_general(
        factors, rho_local, (((1, 2), (1, 2)), ((), ())), preferred_element_type=F32
    )
    slab = rho[:, 0, :].astype(F32)
    la = flat(me, factors)
    di = lax.dynamic_slice_in_dim(damping, pair_at * rows, rows, 0) + damping[0]
    dl = lax.dynamic_slice_in_dim(damping, idx_at * cols, cols, 0).reshape(1, cols)
    b = base(me, e, ham, damping.reshape(width, 1), dl, di.reshape(rows, 1, 1))
    lt = turn(me, la)

    theirs = project(me, la, w, z, slab, True, BF16)
    theirs = swap(theirs, 1)
    mine = project(me, la, w, z, slab, False, F32)
    share = (mine + theirs.astype(F32)).astype(BF16).reshape(16, 64, 1024)
    share = to_owner(share, plane)
    share = jnp.sum(share.astype(F32), axis=0).astype(BF16)
    shares = [share] + [across(share, s) for s in (1, 2, 3)]
    aux = sum(v.astype(F32) for v in shares).astype(BF16)

    aux = jnp.broadcast_to(aux[None], (16, 64, 1024))
    own = to_owner(aux, plane).reshape(1024, 1024)
    oth = swap(own, 1)

    mixed_own, mixed_oth = mix(me, part_own, part_oth, ham)
    mixed_oth = lax.ppermute(mixed_oth, "zl", [(0, 1), (1, 0)])
    term_own = to_owner(mixed_own, plane)
    term_oth = to_owner(mixed_oth, plane)

    out_far = []
    for h in range(2):
        r2, r3 = second(me, lt, own, oth, w, ham, True, h, 1 + 2 * h)
        out_far.append((swap(r2, 2), swap(r3, 3)))
    r0, r1 = second(me, lt, own, oth, w, ham, False, 0, 4)
    r1 = swap(r1, 1)
    pieces = [r0, r1, *[out_far[h][s] for s in range(2) for h in range(2)]]
    out = finish(me, b, term_own, pieces, False, None)
    out = finish(me, b, term_oth, pieces, True, out)
    return out.reshape(rows, width, 2, 1, cols)


def solution(mesh):
    fine = Mesh(mesh.devices.reshape(4, 4, 2, 2, 2), ("x", "y", "zl", "zh", "c"))
    pair, idx = ("x", "y", "zl"), ("zh", "c")
    placed = (P(pair, None, None, None, idx), P(), P(), P(), P(), P(None, pair, idx), P())
    return jax.shard_map(
        per_device,
        mesh=fine,
        in_specs=placed,
        out_specs=P(pair, None, None, None, idx),
        check_vma=False,
    )
```
